32 devices in a mesh: dp: 8 (over z, x), expert: 4 (over y, core).
Axes of the slice: x: 2, y: 2, z: 4, core: 2. Of those that a mesh axis runs over, the one named last changes fastest.
Arguments:
- residual: bfloat16 [32, 4096], P(('dp', 'expert')), may hold values from -6 to 6
- norm_gain: float32 [4096], replicated, may hold values from 0.5 to 1.5
- w_gate: bfloat16 [8, 4096, 9216], P('expert', None, 'dp'), may hold values from -0.09375 to 0.09375
- w_up: bfloat16 [8, 4096, 9216], P('expert', None, 'dp'), may hold values from -0.09375 to 0.09375
- w_down: bfloat16 [8, 9216, 4096], P('expert', 'dp'), may hold values from -0.0625 to 0.0625
- routes: int32 [32, 2], P(('dp', 'expert')), may hold values from 0 to 7, all different within a row; in each aligned block of 4 rows (0 to 3, 4 to 7, ...) at most 2 rows name the same one
- gate_weights: float32 [32, 2], P(('dp', 'expert')), may hold values from 0.2 to 1
- valid_mask: int32 [32], P(('dp', 'expert')), may hold values 0 or 1
- keep_group: int32 [8], P('dp'), may hold values 0 or 1
- grad_out: bfloat16 [32, 4096], P(('dp', 'expert')), may hold values from -64 to 64
Outputs:
- grad_residual: float32 [32, 4096], P(('dp', 'expert'))
- gain_update: float32 [4096], replicated
- gate_update: bfloat16 [8, 4096, 9216], P('expert', None, 'dp')
- up_update: bfloat16 [8, 4096, 9216], P('expert', None, 'dp')
- down_update: bfloat16 [8, 9216, 4096], P('expert', 'dp')
The draws below stay inside these ranges and needn't reach their ends.
Inputs may be any that keep to these rules, and one draw needn't show every extreme that they name: `routes`: each row names 2 different experts. In each aligned block of 4 rows (one data group's tokens) no expert is named by more than 2 rows, and in every draw some expert is named by exactly 2 rows of some block.
All inputs are finite; a program needn't handle non-finite values. No bound on the sum of `valid_mask` or of `keep_group` on one device may be relied on, other than what follows from the above.
Results may differ from the reference program's by a relative error of at most 0.0072.
Values may be sent and summed in bfloat16 or wider, within the bound.
A program may use at most 320 MiB of HBM per device.

```python
import math
import jax
import jax.numpy as jnp
import numpy as np
from jax import lax

D = 4096
FF = 9216
NE = 8
TOP = 2
TOK_DEV = 1
CAP = 2
TOKENS = 32
N_DP = 8
N_EXPERT = 4


def plant(result, own_key, least, high):
    index_at = [jax.random.randint(jax.random.fold_in(own_key, axis), (), 0, length) for axis, length in enumerate(result.shape)]
    longest = result.shape.index(max(result.shape))
    beside = index_at[:longest] + [(index_at[longest] + 1) % result.shape[longest]] + index_at[longest + 1:]
    return result.at[tuple(index_at)].set(least).at[tuple(beside)].set(high)


def shard_levels(rng, extent, pieces, low, largest):
    def one(axis_at, blocks):
        heights = jax.random.uniform(jax.random.fold_in(jax.random.fold_in(rng, 6), axis_at), (blocks,), jnp.float32, low / len(pieces), largest / len(pieces))
        return jnp.repeat(jnp.exp(heights), extent[axis_at] // blocks).reshape((-1,) + (1,) * (len(extent) - axis_at - 1))

    loudness = one(*pieces[0])
    for cut in pieces[1:]:
        loudness = loudness * one(*cut)
    return loudness


def deal_out(stream_key, own, number, rows, count, top, bound, skew):
    sequence = jax.random.permutation(stream_key, count)
    heavy_load, common = portions_of(count, rows * top, bound, skew, True), portions_of(count, rows * top, bound, skew, False)
    places = jnp.arange(count)

    def named(tallies, turn):
        used = int((tallies > 0).sum())
        fixed = max(1, used // 4)
        moved = fixed + (places - fixed + turn * (used - fixed)) % max(1, count - fixed)
        return jnp.zeros((count,), jnp.int32).at[sequence[jnp.where(places < fixed, places, moved)]].set(jnp.asarray(tallies, jnp.int32))

    tallies = jnp.where(number % 4 == 0, named(heavy_load, number // 4), named(common, number - number // 4 - 1))
    mixed = jax.random.permutation(jax.random.fold_in(own, 3), count)
    giver, sink = mixed[0:count // 2 * 2:2], mixed[1:count // 2 * 2:2]
    margin = jnp.minimum(tallies[giver] - 1, bound - tallies[sink]) // 2
    margin = jnp.where((giver == sequence[0]) | (sink == sequence[0]) | (tallies[sink] == 0), 0, jnp.maximum(margin, 0))
    moved = jax.random.randint(jax.random.fold_in(own, 4), (count // 2,), 0, 1 << 20) % (margin + 1)
    tallies = tallies.at[giver].add(-moved).at[sink].add(moved)
    labels = jnp.searchsorted(jnp.cumsum(tallies), jnp.arange(rows * top), side="right").astype(jnp.int32)
    table = labels.reshape(top, rows).T
    table = table[jax.random.permutation(jax.random.fold_in(own, 1), rows)]
    turn = jax.random.randint(jax.random.fold_in(own, 2), (rows, 1), 0, top)
    return jnp.take_along_axis(table, (jnp.arange(top)[None, :] + turn) % top, axis=1)


def portions_of(amount, total, most, skew, full):
    weights = [(1 << 20) // math.isqrt(rank ** skew) + 1 for rank in range(1, amount + 1)]
    largest = most if full else min(most, max(-(-total // amount), total * weights[0] // sum(weights)))
    least = 1 if total - largest >= amount - 1 else 0
    holding, surplus = [largest] + [least] * (amount - 1), total - largest - least * (amount - 1)
    while surplus > 0:
        movable = [i for i in range(1, amount) if holding[i] < largest] or [i for i in range(1, amount) if holding[i] < most]
        whole, remaining = sum([weights[i] for i in movable]), surplus
        for i in movable:
            extra = min(most - holding[i], max(1, remaining * weights[i] // whole), surplus)
            holding[i] = holding[i] + extra
            surplus = surplus - extra
    return np.array(holding)


def centred(stream_key, extent, deviation, most, pieces=(), kind=jnp.bfloat16):
    result = jax.random.normal(stream_key, extent, jnp.float32) * deviation
    if len(pieces) > 0:
        result = shard_levels(stream_key, extent, pieces, -0.22, 0.18) * result
    return jnp.clip(result, min=-most, max=most).astype(kind)


def setup_inputs(seed: int = 0) -> dict:
    streams_of = jax.random.split(jax.random.key(seed), 11)
    residual = centred(streams_of[0], (TOKENS, D), 1.0, 6.0, ((0, 32),))
    norm_gain = jnp.clip(1.0 + 0.1 * jax.random.normal(streams_of[1], (D,), jnp.float32), 0.5, 1.5)
    w_gate = centred(streams_of[2], (NE, D, FF), D ** -0.5, 0.09375, ((0, 4), (2, 8)))
    w_up = centred(streams_of[3], (NE, D, FF), D ** -0.5, 0.09375, ((0, 4), (2, 8)))
    w_down = centred(streams_of[4], (NE, FF, D), FF ** -0.5, 0.0625, ((0, 4), (1, 8)))
    routes_keys = jax.random.split(jax.random.fold_in(streams_of[5], 1), TOKENS // (N_EXPERT * TOK_DEV))
    routes_turns = jax.random.permutation(jax.random.fold_in(streams_of[5], 3), TOKENS // (N_EXPERT * TOK_DEV))
    routes = jax.vmap(lambda own, number: deal_out(jax.random.fold_in(streams_of[5], 2), own, number, N_EXPERT * TOK_DEV, NE, TOP, CAP, 2))(routes_keys, routes_turns).reshape((TOKENS, TOP))
    gate_weights = jnp.clip(0.2 + 0.8 * jax.random.uniform(streams_of[6], (TOKENS, TOP), jnp.float32) ** shard_levels(streams_of[6], (TOKENS, TOP), ((0, 32),), -0.2, 0.2), 0.2, 1.0)
    valid_mask = plant((jax.random.randint(streams_of[7], (TOKENS,), 0, 4) < 3).astype(jnp.int32), jax.random.fold_in(streams_of[7], 1), 0, 1)
    keep_group = plant((jax.random.randint(streams_of[8], (N_DP,), 0, 2) < 1).astype(jnp.int32), jax.random.fold_in(streams_of[8], 1), 0, 1)
    grad_out = centred(streams_of[9], (TOKENS, D), (TOKENS // 3), 64.0, ((0, 32),))
    return dict(residual=residual, norm_gain=norm_gain, w_gate=w_gate, w_up=w_up, w_down=w_down, routes=routes, gate_weights=gate_weights, valid_mask=valid_mask, keep_group=keep_group, grad_out=grad_out)


norm_eps = 1e-05

def expert_rows(expert_id, routes, gate_weights):
    hits = routes == expert_id
    weight = lax.optimization_barrier(jnp.sum(jnp.where(hits, gate_weights, jnp.zeros_like(gate_weights)), axis=1))
    flagged = jnp.any(hits, axis=1)
    order = jnp.argsort(jnp.where(flagged, 0, 1).astype(jnp.int32), stable=True)
    return (order[:N_DP * CAP].astype(jnp.int32), weight)

def expert_math(inputs, cotangent, gate_mat, up_mat, down_mat):
    gate_pre = jnp.dot(inputs, gate_mat, preferred_element_type=jnp.float32)
    up_pre = jnp.dot(inputs, up_mat, preferred_element_type=jnp.float32)
    sigma = jax.nn.sigmoid(gate_pre)
    active = gate_pre * sigma
    hidden = (active * up_pre).astype(jnp.bfloat16)
    back_h = jnp.dot(cotangent, down_mat.T, preferred_element_type=jnp.float32)
    d_up = (back_h * active).astype(jnp.bfloat16)
    d_gate = (back_h * up_pre * sigma * (1.0 + gate_pre * (1.0 - sigma))).astype(jnp.bfloat16)
    grad_gate = jnp.dot(inputs.T, d_gate, preferred_element_type=jnp.float32)
    grad_up = jnp.dot(inputs.T, d_up, preferred_element_type=jnp.float32)
    grad_down = jnp.dot(hidden.T, cotangent, preferred_element_type=jnp.float32)
    return (grad_gate, grad_up, grad_down, d_gate, d_up)

def reference(residual, norm_gain, w_gate, w_up, w_down, routes, gate_weights, valid_mask, keep_group, grad_out):
    wide = residual.astype(jnp.float32)
    inv_rms = lax.rsqrt(lax.optimization_barrier(jnp.mean(wide * wide, axis=1, keepdims=True)) + norm_eps)
    normed = wide * inv_rms
    normed_in = (normed * norm_gain).astype(jnp.bfloat16)
    group_of = (jnp.arange(TOKENS) // (TOK_DEV * N_EXPERT)).astype(jnp.int32)
    live = valid_mask * keep_group[group_of]
    count = jnp.maximum(jnp.sum(live).astype(jnp.float32), 1.0)
    masked_grad = jnp.where(live[:, None] > 0, grad_out, jnp.zeros_like(grad_out))

    def pick(expert_id):
        order, weight = expert_rows(expert_id, routes, gate_weights)
        inputs = normed_in[order]
        cotangent = (weight[order][:, None] * masked_grad[order].astype(jnp.float32)).astype(jnp.bfloat16)
        return (order, inputs, cotangent)

    def first_pass(carry, expert_id):
        back_sum, squares = carry
        order, inputs, cotangent = pick(expert_id)
        gate_mat = w_gate[expert_id]
        up_mat = w_up[expert_id]
        grad_gate, grad_up, grad_down, d_gate, d_up = expert_math(inputs, cotangent, gate_mat, up_mat, w_down[expert_id])
        back_x = jnp.dot(d_gate, gate_mat.T, preferred_element_type=jnp.float32) + jnp.dot(d_up, up_mat.T, preferred_element_type=jnp.float32)
        squares = squares + jnp.sum(grad_gate * grad_gate) + jnp.sum(grad_up * grad_up) + jnp.sum(grad_down * grad_down)
        back_sum = back_sum.at[order].add(back_x)
        return ((back_sum, squares), None)
    start = (jnp.zeros((TOKENS, D), jnp.float32), jnp.zeros((), jnp.float32))
    (back_in, squares), _ = lax.scan(first_pass, start, jnp.arange(NE, dtype=jnp.int32))
    gain_grad = lax.optimization_barrier(jnp.sum(back_in * normed, axis=0)) / count
    back_n = back_in * norm_gain
    grad_residual = inv_rms * (back_n - normed * lax.optimization_barrier(jnp.mean(back_n * normed, axis=1, keepdims=True))) / count
    total = squares / (count * count) + jnp.sum(gain_grad * gain_grad)
    param_total = float(3 * NE * D * FF + D)
    factor = 1.0 / jnp.maximum(jnp.sqrt(total / param_total), 1.0)
    scale = factor / count

    def second_pass(expert_id):
        order, inputs, cotangent = pick(expert_id)
        grad_gate, grad_up, grad_down, d_gate, d_up = expert_math(inputs, cotangent, w_gate[expert_id], w_up[expert_id], w_down[expert_id])
        return ((grad_gate * scale).astype(jnp.bfloat16), (grad_up * scale).astype(jnp.bfloat16), (grad_down * scale).astype(jnp.bfloat16))
    gate_update, up_update, down_update = lax.map(second_pass, jnp.arange(NE, dtype=jnp.int32))
    return (grad_residual, gain_grad * factor, gate_update, up_update, down_update)
```

```python
import functools

import jax
import jax.numpy as jnp
from jax import lax
from jax.experimental import pallas as pl
from jax.experimental.pallas import tpu as pltpu
from jax.sharding import PartitionSpec as P

D = 4096
FF = 9216
NE = 8
CAP = 2


norm_eps = 1e-05


def shards_plain(
    residual,
    norm_gain,
    w_gate,
    w_up,
    w_down,
    routes,
    gate_weights,
    valid_mask,
    keep_group,
    grad_out,
):
    wide = residual.astype(jnp.float32)
    inv_rms = lax.rsqrt(jnp.mean(wide * wide, axis=1, keepdims=True) + norm_eps)
    normed = wide * inv_rms
    normed_in = (normed * norm_gain).astype(jnp.bfloat16)
    live = valid_mask * keep_group[0]
    local_count = jnp.sum(live).astype(jnp.float32)
    masked_grad = jnp.where(live[:, None] > 0, grad_out, jnp.zeros_like(grad_out))
    peers = lax.axis_size("expert")
    per_dev = w_gate.shape[0]
    tok_rows = residual.shape[0]
    width = residual.shape[1]
    expert_ids = jnp.arange(peers * per_dev, dtype=jnp.int32).reshape(peers, per_dev)
    hits = routes[None, None, :, :] == expert_ids[:, :, None, None]
    weight = jnp.sum(jnp.where(hits, gate_weights[None, None], jnp.zeros((), jnp.float32)), axis=3)
    flagged = jnp.any(hits, axis=3)
    send_in = jnp.where(flagged[..., None], normed_in[None, None], jnp.zeros((), jnp.bfloat16))
    send_grad = (weight[..., None] * masked_grad[None, None].astype(jnp.float32)).astype(
        jnp.bfloat16
    )
    send_flag = flagged.astype(jnp.bfloat16)
    got_in, got_grad, got_flag = (
        lax.all_to_all(send_in, "expert", split_axis=0, concat_axis=0, tiled=True),
        lax.all_to_all(send_grad, "expert", split_axis=0, concat_axis=0, tiled=True),
        lax.all_to_all(send_flag, "expert", split_axis=0, concat_axis=0, tiled=True),
    )
    group_rows = peers * tok_rows
    cand_in = jnp.transpose(got_in, (1, 0, 2, 3)).reshape(per_dev, group_rows, width)
    cand_grad = jnp.transpose(got_grad, (1, 0, 2, 3)).reshape(per_dev, group_rows, width)
    flag_rows = jnp.transpose(got_flag, (1, 0, 2)).reshape(per_dev, group_rows).astype(jnp.int32)
    ranks = jnp.cumsum(flag_rows, axis=1) - flag_rows
    slot_ids = jnp.arange(CAP, dtype=jnp.int32)
    picker = ((flag_rows[:, None, :] > 0) & (ranks[:, None, :] == slot_ids[None, :, None])).astype(
        jnp.bfloat16
    )
    rows_in = jnp.einsum(
        "lcq,lqd->cld", picker, cand_in, preferred_element_type=jnp.float32
    ).astype(jnp.bfloat16)
    rows_grad = jnp.einsum(
        "lcq,lqd->cld", picker, cand_grad, preferred_element_type=jnp.float32
    ).astype(jnp.bfloat16)
    all_in, all_grad = (
        lax.all_gather(rows_in, "dp", axis=0, tiled=True),
        lax.all_gather(rows_grad, "dp", axis=0, tiled=True),
    )
    gate_pre = jnp.einsum("rld,ldf->rlf", all_in, w_gate, preferred_element_type=jnp.float32)
    up_pre = jnp.einsum("rld,ldf->rlf", all_in, w_up, preferred_element_type=jnp.float32)
    sigma = jax.nn.sigmoid(gate_pre)
    active = gate_pre * sigma
    hidden = (active * up_pre).astype(jnp.bfloat16)
    back_h = jnp.einsum("rld,lfd->rlf", all_grad, w_down, preferred_element_type=jnp.float32)
    d_up = (back_h * active).astype(jnp.bfloat16)
    d_gate = (back_h * up_pre * sigma * (1.0 + gate_pre * (1.0 - sigma))).astype(jnp.bfloat16)
    grad_gate = jnp.einsum("rld,rlf->ldf", all_in, d_gate, preferred_element_type=jnp.float32)
    grad_up = jnp.einsum("rld,rlf->ldf", all_in, d_up, preferred_element_type=jnp.float32)
    grad_down = jnp.einsum("rlf,rld->lfd", hidden, all_grad, preferred_element_type=jnp.float32)
    first = jnp.einsum("rlf,ldf->rld", d_gate, w_gate, preferred_element_type=jnp.float32)
    back_mine = lax.psum_scatter(
        first + jnp.einsum("rlf,ldf->rld", d_up, w_up, preferred_element_type=jnp.float32),
        "dp",
        scatter_dimension=0,
        tiled=True,
    )
    back_cand = jnp.einsum(
        "lcq,cld->lqd", picker.astype(jnp.float32), back_mine, precision=lax.Precision.HIGHEST
    )
    back_send = jnp.transpose(back_cand.reshape(per_dev, peers, tok_rows, width), (1, 0, 2, 3))
    back_got = lax.all_to_all(back_send, "expert", split_axis=0, concat_axis=0, tiled=True)
    back_in = jnp.sum(back_got, axis=(0, 1))
    gain_local = jnp.sum(back_in * normed, axis=0)
    back_n = back_in * norm_gain
    grad_core = inv_rms * (back_n - normed * jnp.mean(back_n * normed, axis=1, keepdims=True))
    param_total = float(3 * NE * D * FF + D)
    local_sq = (
        jnp.sum(grad_gate * grad_gate) + jnp.sum(grad_up * grad_up) + jnp.sum(grad_down * grad_down)
    )
    count_all, gain_all, squares_all = lax.psum(
        (local_count, gain_local, local_sq), ("dp", "expert")
    )
    count = jnp.maximum(count_all, 1.0)
    gain_grad = gain_all / count
    total = squares_all / (count * count) + jnp.sum(gain_grad * gain_grad)
    factor = 1.0 / jnp.maximum(jnp.sqrt(total / param_total), 1.0)
    scale = factor / count
    grad_residual = grad_core / count
    gate_update = (grad_gate * scale).astype(jnp.bfloat16)
    up_update = (grad_up * scale).astype(jnp.bfloat16)
    down_update = (grad_down * scale).astype(jnp.bfloat16)
    return (grad_residual, gain_grad * factor, gate_update, up_update, down_update)

MESH = pl.DeviceIdType.MESH
VMEM = pl.BlockSpec(memory_space=pltpu.VMEM)
HBM = pl.BlockSpec(memory_space=pl.ANY)
NT = (((1,), (1,)), ((), ()))
F32 = dict(preferred_element_type=jnp.float32)
LOADS = 4
STEPS = 8


def front_kernel(
    n_dp, n_expert, param_total, chunk,
    res_ref, grad_ref, routes_ref, gates_ref, valid_ref, keep_ref, gain_ref,
    wg_ref, wu_ref, wd_ref,
    xt_out, c_out, dgu_out, ht_out, core_out, gain_out, scale_out,
    gu, wd, rows, land_x, land_g, land_m, x_ref, normed, pre, back_h, hid_ref, back,
    land_eb, stage, land_row, msg, land_msg, land_gain, gain_part,
    w_sem, d_sem, x_send, x_recv, x_fwd, m_send, m_recv,
    eb_send, eb_recv, row_send, row_recv, g_send, g_recv,
):
    n = n_dp * n_expert
    d, e = lax.axis_index("dp"), lax.axis_index("expert")
    me = e * n_dp + d
    per_dev, width, two_hid = gu.shape
    hid = two_hid // 2
    lanes = width // 128
    n_chunks = width // chunk

    def load_gu(l, p):
        size = width // LOADS
        at = pl.ds(p * size, size)
        return (
            pltpu.make_async_copy(wg_ref.at[l, at, :], gu.at[l, at, pl.ds(0, hid)], w_sem.at[l, 0, p]),
            pltpu.make_async_copy(wu_ref.at[l, at, :], gu.at[l, at, pl.ds(hid, hid)], w_sem.at[l, 1, p]),
        )

    def load_wd(l, p):
        size = hid // LOADS
        at = pl.ds(p * size, size)
        return pltpu.make_async_copy(wd_ref.at[l, at, :], wd.at[at, :], d_sem.at[l, p])

    def start_gu(l):
        for p in range(LOADS):
            for copy in load_gu(l, p):
                copy.start()

    def start_wd(l):
        for p in range(LOADS):
            load_wd(l, p).start()

    start_gu(0)
    start_wd(0)

    wide = res_ref[...].astype(jnp.float32)
    inv_rms = lax.rsqrt(jnp.mean(wide * wide, axis=1, keepdims=True) + norm_eps)
    grad = grad_ref[...].astype(jnp.float32)
    for j in range(lanes):
        at = slice(j * 128, (j + 1) * 128)
        rows[j : j + 1, :] = wide[:, at]
        rows[lanes + j : lanes + j + 1, :] = grad[:, at]
    land_x[me] = rows[:lanes].astype(jnp.bfloat16)
    land_g[me] = rows[lanes : 2 * lanes].astype(jnp.bfloat16)
    lane = lax.broadcasted_iota(jnp.int32, (1, 128), 1)
    parts = (
        routes_ref[:, 0:1].astype(jnp.float32),
        routes_ref[:, 1:2].astype(jnp.float32),
        gates_ref[:, 0:1],
        gates_ref[:, 1:2],
        (valid_ref[...] * keep_ref[...]).astype(jnp.float32),
        inv_rms,
    )
    meta = jnp.zeros((1, 128), jnp.float32)
    for at, part in enumerate(parts):
        meta = jnp.where(lane == at, part, meta)
    land_m[me] = meta

    def place(row):
        return {"dp": row % n_dp, "expert": row // n_dp}

    others = [(me + k) % n for k in range(1, n)]
    barrier = pltpu.get_barrier_semaphore()
    for row in others:
        pl.semaphore_signal(barrier, inc=1, device_id=place(row), device_id_type=MESH)
    pl.semaphore_wait(barrier, n - 1)

    def remote(src, dst, send, recv, where):
        return pltpu.make_async_remote_copy(
            src_ref=src, dst_ref=dst, send_sem=send, recv_sem=recv,
            device_id=where, device_id_type=MESH,
        )

    half = n_expert // 2
    mate = e + 1 - 2 * (e % 2)
    same = [
        ((d + k // half) % n_dp, (e + 2 * (k % half)) % n_expert) for k in range(1, n_dp * half)
    ]
    cross = [(d, mate)] + [(pd, pe + 1 - 2 * (pe % 2)) for pd, pe in same]

    def direct(i, land, k, row):
        pd, pe = same[k]
        return remote(
            land.at[row], land.at[row], x_send.at[i, k], x_recv.at[i, row], {"dp": pd, "expert": pe}
        )

    def forward(i, land, k, row):
        return remote(
            land.at[row], land.at[row], x_fwd.at[i, k], x_recv.at[i, row], {"expert": mate}
        )

    def meta_copy(k, row):
        return remote(land_m.at[row], land_m.at[row], m_send.at[k], m_recv.at[row], place(others[k]))

    lands = (land_x, land_g)
    for i, land in enumerate(lands):
        for k in range(len(same)):
            direct(i, land, k, me).start()
        forward(i, land, 0, me).start()
        if i == 0:
            for k in range(n - 1):
                meta_copy(k, me).start()

    def relay(i, land):
        for k, (pd, pe) in enumerate(same):
            row = pe * n_dp + pd
            direct(i, land, k, row).wait_recv()
            forward(i, land, k + 1, row).start()

    def finish(i, land):
        for pd, pe in cross:
            row = pe * n_dp + pd
            forward(i, land, 0, row).wait_recv()

    relay(0, land_x)
    finish(0, land_x)
    for k in range(n - 1):
        meta_copy(k, others[k]).wait_recv()
    relay(1, land_g)
    finish(1, land_g)

    start_gu(1)

    meta_all = land_m[:, 0, :]
    inv_all = meta_all[:, 5:6]

    def spread(land):
        for r in range(n):
            rows[r * lanes : (r + 1) * lanes, :] = land[r].astype(jnp.float32)

    spread(land_x)
    for j in range(lanes):
        at = slice(j * 128, (j + 1) * 128)
        part = rows[pl.ds(j, n, stride=lanes), :] * inv_all
        normed[:, at] = part
        x_ref[:, at] = (part * gain_ref[:, at]).astype(jnp.bfloat16)
    spread(land_g)
    alive = meta_all[:, 4:5] > 0
    weights = []
    for l in range(per_dev):
        own = (e * per_dev + l).astype(jnp.float32)
        weights.append(
            jnp.where(meta_all[:, 0:1] == own, meta_all[:, 2:3], 0.0)
            + jnp.where(meta_all[:, 1:2] == own, meta_all[:, 3:4], 0.0)
        )
    for j in range(lanes):
        at = slice(j * 128, (j + 1) * 128)
        part = jnp.where(alive, rows[pl.ds(j, n, stride=lanes), :], 0.0)
        for l in range(per_dev):
            c_out[l, :, at] = (weights[l] * part).astype(jnp.bfloat16)

    squares = jnp.zeros((1, 1), jnp.float32)
    gram_x = lax.dot_general(x_ref[...], x_ref[...], NT, **F32)
    fwd_tile = next(t for t in (768, 512, 256) if two_hid % t == 0)
    mine = pl.multiple_of(e * n_dp, n_dp)

    def eb_copy(ci, pe, slot):
        cols = pl.ds(pl.multiple_of(ci * chunk, chunk), chunk)
        return remote(
            back.at[pl.ds(pl.multiple_of(pe * n_dp, n_dp), n_dp), cols],
            land_eb.at[slot, :, cols], eb_send.at[ci, pe], eb_recv.at[ci, slot], {"expert": pe},
        )

    def row_copy(ci, pd, slot):
        cols = pl.ds(pl.multiple_of(ci * chunk, chunk), chunk)
        return remote(
            stage.at[pd, :, cols], land_row.at[slot, :, cols],
            row_send.at[ci, pd], row_recv.at[ci, slot], {"dp": pd},
        )

    e_peers = [(e + k) % n_expert for k in range(1, n_expert)]
    d_peers = [(d + k) % n_dp for k in range(1, n_dp)]

    def fold(ci):
        cols = pl.ds(pl.multiple_of(ci * chunk, chunk), chunk)
        for pe in e_peers:
            eb_copy(ci, pe, pe).wait_recv()
        group = jnp.sum(land_eb[:, :, cols], axis=0)
        for k in range(n_dp):
            stage[k, :, cols] = group[k : k + 1]
        land_row[d, :, cols] = stage[d, :, cols]
        for pd in d_peers:
            row_copy(ci, pd, d).start()

    for l in range(per_dev):
        for p in range(LOADS):
            for copy in load_gu(l, p):
                copy.wait()

        def fwd(t, _):
            cols = pl.ds(pl.multiple_of(t * fwd_tile, fwd_tile), fwd_tile)
            pre[:, cols] = jnp.dot(x_ref[...], gu[l, :, cols], **F32)
            return 0

        lax.fori_loop(0, two_hid // fwd_tile, fwd, 0)
        for p in range(LOADS):
            load_wd(l, p).wait()
        back_h[...] = jnp.zeros_like(back_h)

        def down(t, _):
            cols = pl.ds(pl.multiple_of(t * 1024, 1024), 1024)
            back_h[...] += lax.dot_general(c_out[l, :, cols], wd[:, cols], NT, **F32)
            return 0

        lax.fori_loop(0, width // 1024, down, 0)
        if l + 1 < per_dev:
            start_wd(l + 1)
        for j in range(hid // 128):
            at = slice(j * 128, (j + 1) * 128)
            up_at = slice(hid + j * 128, hid + (j + 1) * 128)
            gate_pre, up_pre, down_in = pre[:, at], pre[:, up_at], back_h[:, at]
            sigma = jax.nn.sigmoid(gate_pre)
            active = gate_pre * sigma
            hid_ref[:, at] = (active * up_pre).astype(jnp.bfloat16)
            dgu_out[l, :, up_at] = (down_in * active).astype(jnp.bfloat16)
            dgu_out[l, :, at] = (
                down_in * up_pre * sigma * (1.0 + gate_pre * (1.0 - sigma))
            ).astype(jnp.bfloat16)

        last = l + 1 == per_dev

        def back_step(ci, _):
            cols = pl.ds(pl.multiple_of(ci * chunk, chunk), chunk)
            part = lax.dot_general(dgu_out[l], gu[l, cols, :], NT, **F32)
            if l > 0:
                part += back[:, cols]
            back[:, cols] = part
            if last:
                gain_part[:, cols] = jnp.sum(part * normed[:, cols], axis=0, keepdims=True)
                land_eb[e, :, cols] = back[pl.ds(mine, n_dp), cols]
                for pe in e_peers:
                    eb_copy(ci, pe, e).start()

                @pl.when(ci >= 2)
                def _():
                    fold(ci - 2)

            return 0

        lax.fori_loop(0, n_chunks, back_step, 0)
        dgu, hidden, c = dgu_out[l], hid_ref[...], c_out[l]
        terms = lax.dot_general(dgu, dgu, NT, **F32) * gram_x + lax.dot_general(
            hidden, hidden, NT, **F32
        ) * lax.dot_general(c, c, NT, **F32)
        squares += jnp.sum(jnp.sum(terms, axis=1, keepdims=True), axis=0, keepdims=True)
        ht_out[l] = hidden.T

    piece = width // n
    for k in range(n):
        msg[k, :, :piece] = gain_part[:, k * piece : (k + 1) * piece]
        msg[k, :, piece:] = jnp.broadcast_to(squares, (1, 128))

    def msg_copy(k, slot):
        return remote(msg.at[others[k]], land_msg.at[slot], g_send.at[0, k], g_recv.at[0, slot], place(others[k]))

    def gain_copy(k, slot):
        return remote(
            land_gain.at[slot], land_gain.at[slot], g_send.at[1, k], g_recv.at[1, slot], place(others[k])
        )

    for k in range(n - 1):
        msg_copy(k, me).start()
    land_msg[me] = msg[me]
    for ci in range(max(0, n_chunks - 2), n_chunks):
        fold(ci)
    xt_out[...] = x_ref[...].T
    for k in range(n - 1):
        msg_copy(k, others[k]).wait_recv()
    total = jnp.sum(land_msg[...], axis=0)
    land_gain[me] = total[:, :piece]
    for k in range(n - 1):
        gain_copy(k, me).start()

    count = jnp.maximum(jnp.sum(land_m[:, :, 4:5]), 1.0)
    for ci in range(n_chunks):
        for pd in d_peers:
            row_copy(ci, pd, pd).wait_recv()
    own_wide = res_ref[...].astype(jnp.float32)
    own_inv = lax.rsqrt(jnp.mean(own_wide * own_wide, axis=1, keepdims=True) + norm_eps)
    own_normed = own_wide * own_inv
    back_n = jnp.sum(land_row[...], axis=0) * gain_ref[...]
    core = own_inv * (back_n - own_normed * jnp.mean(back_n * own_normed, axis=1, keepdims=True))
    core_out[...] = core / count

    for k in range(n - 1):
        gain_copy(k, others[k]).wait_recv()
    gain_grad = land_gain[...] / count
    whole = total[:, piece : piece + 1] / (count * count) + jnp.sum(gain_grad * gain_grad)
    factor = 1.0 / jnp.maximum(jnp.sqrt(whole / param_total), 1.0)
    gain_out[...] = gain_grad * factor
    scale_out[...] = jnp.broadcast_to(factor / count, scale_out.shape)

    for i, land in enumerate(lands):
        for k in range(len(same)):
            direct(i, land, k, me).wait_send()
        for k in range(len(same) + 1):
            forward(i, land, k, me).wait_send()
    for k in range(n - 1):
        meta_copy(k, me).wait_send()
        msg_copy(k, me).wait_send()
        gain_copy(k, me).wait_send()
    for ci in range(n_chunks):
        for pe in e_peers:
            eb_copy(ci, pe, e).wait_send()
        for pd in d_peers:
            row_copy(ci, pd, d).wait_send()


def update_kernel(
    xt_ref, c_ref, dgu_ref, ht_ref, core_ref, gain_ref, scale_ref,
    resid_out, gain_out, og_ref, ou_ref, od_ref,
):
    @pl.when((pl.program_id(0) == 0) & (pl.program_id(1) == 0))
    def _():
        resid_out[...] = core_ref[...]
        piece = gain_ref.shape[2]
        for k in range(gain_ref.shape[0]):
            gain_out[:, k * piece : (k + 1) * piece] = gain_ref[k]

    scale = scale_ref[:, 0:1]
    hid = og_ref.shape[2]
    width = od_ref.shape[2]
    for at in range(0, 2 * hid, 256):
        size = min(256, 2 * hid - at)
        part = jnp.dot(xt_ref[...], dgu_ref[0, :, at : at + size], **F32) * scale
        part = part.astype(jnp.bfloat16)
        for k in range(0, size, 128):
            col = at + k
            ref, col = (og_ref, col) if col < hid else (ou_ref, col - hid)
            ref[0, :, col : col + 128] = part[:, k : k + 128]
    for at in range(0, width, 256):
        part = jnp.dot(ht_ref[0], c_ref[0, :, at : at + 256], **F32) * scale
        od_ref[0, :, at : at + 256] = part.astype(jnp.bfloat16)


def shards_kernel(
    n_dp,
    n_expert,
    residual,
    norm_gain,
    w_gate,
    w_up,
    w_down,
    routes,
    gate_weights,
    valid_mask,
    keep_group,
    grad_out,
):
    n = n_dp * n_expert
    per_dev, width, hid = w_gate.shape
    lanes = width // 128
    piece = width // n
    chunk = width // 8
    n_chunks = width // chunk
    param_total = float(3 * n_expert * per_dev * width * hid * n_dp + width)
    bf = lambda *shape: pltpu.VMEM(shape, jnp.bfloat16)
    vec = lambda *shape: pltpu.VMEM(shape, jnp.float32)
    dma = lambda *shape: pltpu.SemaphoreType.DMA(shape)
    shape_bf = lambda *shape: jax.ShapeDtypeStruct(shape, jnp.bfloat16)
    shape_f = lambda *shape: jax.ShapeDtypeStruct(shape, jnp.float32)
    same = n_dp * (n_expert // 2)
    xt, c, dgu, ht, core, gain, scale = pl.pallas_call(
        functools.partial(front_kernel, n_dp, n_expert, param_total, chunk),
        out_shape=(
            shape_bf(width, n),
            shape_bf(per_dev, n, width),
            shape_bf(per_dev, n, 2 * hid),
            shape_bf(per_dev, hid, n),
            shape_f(1, width),
            shape_f(n, 1, piece),
            shape_f(1, 128),
        ),
        in_specs=[VMEM] * 7 + [HBM] * 3,
        out_specs=[VMEM] * 7,
        scratch_shapes=[
            bf(per_dev, width, 2 * hid),
            bf(hid, width),
            vec(n * lanes, 128),
            bf(n, lanes, 128),
            bf(n, lanes, 128),
            vec(n, 1, 128),
            bf(n, width),
            vec(n, width),
            vec(n, 2 * hid),
            vec(n, hid),
            bf(n, hid),
            vec(n, width),
            vec(n_expert, n_dp, width),
            vec(n_dp, 1, width),
            vec(n_dp, 1, width),
            vec(n, 1, piece + 128),
            vec(n, 1, piece + 128),
            vec(n, 1, piece),
            vec(1, width),
            dma(per_dev, 2, LOADS),
            dma(per_dev, LOADS),
            dma(2, same),
            dma(2, n),
            dma(2, same),
            dma(n),
            dma(n),
            dma(n_chunks, n_expert),
            dma(n_chunks, n_expert),
            dma(n_chunks, n_dp),
            dma(n_chunks, n_dp),
            dma(2, n),
            dma(2, n),
        ],
        compiler_params=pltpu.CompilerParams(
            collective_id=0, has_side_effects=True, vmem_limit_bytes=60000 * 1024
        ),
        name="front",
    )(
        residual,
        grad_out,
        routes,
        gate_weights,
        valid_mask[None],
        keep_group[None],
        norm_gain[None],
        w_gate,
        w_up,
        w_down,
    )
    whole = lambda *shape: pl.BlockSpec(shape, lambda l, s: (0,) * len(shape))
    block = lambda *shape: pl.BlockSpec((1,) + shape, lambda l, s: (l, s, 0))
    per_expert = lambda *shape: pl.BlockSpec((1,) + shape, lambda l, s: (l, 0, 0))
    size, size_h = width // STEPS, hid // STEPS
    return_shapes = (
        shape_f(1, width),
        shape_f(1, width),
        jax.ShapeDtypeStruct(w_gate.shape, jnp.bfloat16),
        jax.ShapeDtypeStruct(w_up.shape, jnp.bfloat16),
        jax.ShapeDtypeStruct(w_down.shape, jnp.bfloat16),
    )
    grad_residual, gain_update, gate_update, up_update, down_update = pl.pallas_call(
        update_kernel,
        grid=(per_dev, STEPS),
        out_shape=return_shapes,
        in_specs=[
            pl.BlockSpec((size, n), lambda l, s: (s, 0)),
            per_expert(n, width),
            per_expert(n, 2 * hid),
            block(size_h, n),
            whole(1, width),
            whole(n, 1, piece),
            whole(1, 128),
        ],
        out_specs=[
            whole(1, width),
            whole(1, width),
            block(size, hid),
            block(size, hid),
            block(size_h, width),
        ],
        compiler_params=pltpu.CompilerParams(vmem_limit_bytes=40000 * 1024),
        name="update",
    )(xt, c, dgu, ht, core, gain, scale)
    return (grad_residual, gain_update.reshape(width), gate_update, up_update, down_update)


def shards_for(mesh):
    n_dp, n_expert = mesh.shape["dp"], mesh.shape["expert"]

    def run(*args):
        residual, w_gate = args[0], args[2]
        per_dev, width, hid = w_gate.shape
        n = n_dp * n_expert
        fits = (
            residual.shape[0] == 1
            and hid % 128 == 0
            and n <= 64
            and n_dp % 8 == 0
            and n_expert % 2 == 0
            and width % (128 * n) == 0
            and width % 1024 == 0
            and (2 * per_dev + 1) * width * hid * 2 <= 50 * 2**20
        )
        if fits:
            return shards_kernel(n_dp, n_expert, *args)
        return shards_plain(*args)

    return run


def solution(mesh):
    placed = (
        P(("dp", "expert"), None),
        P(),
        P("expert", None, "dp"),
        P("expert", None, "dp"),
        P("expert", "dp", None),
        P(("dp", "expert"), None),
        P(("dp", "expert"), None),
        P(("dp", "expert")),
        P("dp"),
        P(("dp", "expert"), None),
    )
    return jax.shard_map(
        shards_for(mesh),
        mesh=mesh,
        in_specs=placed,
        out_specs=(
            P(("dp", "expert"), None),
            P(),
            P("expert", None, "dp"),
            P("expert", None, "dp"),
            P("expert", "dp", None),
        ),
        check_vma=False,
    )
```

```python
import functools

import jax
import jax.numpy as jnp
from jax import lax
from jax.experimental import pallas as pl
from jax.experimental.pallas import tpu as pltpu
from jax.sharding import PartitionSpec as P

D = 4096
FF = 9216
NE = 8
CAP = 2


norm_eps = 1e-05


def shards_plain(
    residual,
    norm_gain,
    w_gate,
    w_up,
    w_down,
    routes,
    gate_weights,
    valid_mask,
    keep_group,
    grad_out,
):
    wide = residual.astype(jnp.float32)
    inv_rms = lax.rsqrt(jnp.mean(wide * wide, axis=1, keepdims=True) + norm_eps)
    normed = wide * inv_rms
    normed_in = (normed * norm_gain).astype(jnp.bfloat16)
    live = valid_mask * keep_group[0]
    local_count = jnp.sum(live).astype(jnp.float32)
    masked_grad = jnp.where(live[:, None] > 0, grad_out, jnp.zeros_like(grad_out))
    peers = lax.axis_size("expert")
    per_dev = w_gate.shape[0]
    tok_rows = residual.shape[0]
    width = residual.shape[1]
    expert_ids = jnp.arange(peers * per_dev, dtype=jnp.int32).reshape(peers, per_dev)
    hits = routes[None, None, :, :] == expert_ids[:, :, None, None]
    weight = jnp.sum(jnp.where(hits, gate_weights[None, None], jnp.zeros((), jnp.float32)), axis=3)
    flagged = jnp.any(hits, axis=3)
    send_in = jnp.where(flagged[..., None], normed_in[None, None], jnp.zeros((), jnp.bfloat16))
    send_grad = (weight[..., None] * masked_grad[None, None].astype(jnp.float32)).astype(
        jnp.bfloat16
    )
    send_flag = flagged.astype(jnp.bfloat16)
    got_in, got_grad, got_flag = (
        lax.all_to_all(send_in, "expert", split_axis=0, concat_axis=0, tiled=True),
        lax.all_to_all(send_grad, "expert", split_axis=0, concat_axis=0, tiled=True),
        lax.all_to_all(send_flag, "expert", split_axis=0, concat_axis=0, tiled=True),
    )
    group_rows = peers * tok_rows
    cand_in = jnp.transpose(got_in, (1, 0, 2, 3)).reshape(per_dev, group_rows, width)
    cand_grad = jnp.transpose(got_grad, (1, 0, 2, 3)).reshape(per_dev, group_rows, width)
    flag_rows = jnp.transpose(got_flag, (1, 0, 2)).reshape(per_dev, group_rows).astype(jnp.int32)
    ranks = jnp.cumsum(flag_rows, axis=1) - flag_rows
    slot_ids = jnp.arange(CAP, dtype=jnp.int32)
    picker = ((flag_rows[:, None, :] > 0) & (ranks[:, None, :] == slot_ids[None, :, None])).astype(
        jnp.bfloat16
    )
    rows_in = jnp.einsum(
        "lcq,lqd->cld", picker, cand_in, preferred_element_type=jnp.float32
    ).astype(jnp.bfloat16)
    rows_grad = jnp.einsum(
        "lcq,lqd->cld", picker, cand_grad, preferred_element_type=jnp.float32
    ).astype(jnp.bfloat16)
    all_in, all_grad = (
        lax.all_gather(rows_in, "dp", axis=0, tiled=True),
        lax.all_gather(rows_grad, "dp", axis=0, tiled=True),
    )
    gate_pre = jnp.einsum("rld,ldf->rlf", all_in, w_gate, preferred_element_type=jnp.float32)
    up_pre = jnp.einsum("rld,ldf->rlf", all_in, w_up, preferred_element_type=jnp.float32)
    sigma = jax.nn.sigmoid(gate_pre)
    active = gate_pre * sigma
    hidden = (active * up_pre).astype(jnp.bfloat16)
    back_h = jnp.einsum("rld,lfd->rlf", all_grad, w_down, preferred_element_type=jnp.float32)
    d_up = (back_h * active).astype(jnp.bfloat16)
    d_gate = (back_h * up_pre * sigma * (1.0 + gate_pre * (1.0 - sigma))).astype(jnp.bfloat16)
    grad_gate = jnp.einsum("rld,rlf->ldf", all_in, d_gate, preferred_element_type=jnp.float32)
    grad_up = jnp.einsum("rld,rlf->ldf", all_in, d_up, preferred_element_type=jnp.float32)
    grad_down = jnp.einsum("rlf,rld->lfd", hidden, all_grad, preferred_element_type=jnp.float32)
    first = jnp.einsum("rlf,ldf->rld", d_gate, w_gate, preferred_element_type=jnp.float32)
    back_mine = lax.psum_scatter(
        first + jnp.einsum("rlf,ldf->rld", d_up, w_up, preferred_element_type=jnp.float32),
        "dp",
        scatter_dimension=0,
        tiled=True,
    )
    back_cand = jnp.einsum(
        "lcq,cld->lqd", picker.astype(jnp.float32), back_mine, precision=lax.Precision.HIGHEST
    )
    back_send = jnp.transpose(back_cand.reshape(per_dev, peers, tok_rows, width), (1, 0, 2, 3))
    back_got = lax.all_to_all(back_send, "expert", split_axis=0, concat_axis=0, tiled=True)
    back_in = jnp.sum(back_got, axis=(0, 1))
    gain_local = jnp.sum(back_in * normed, axis=0)
    back_n = back_in * norm_gain
    grad_core = inv_rms * (back_n - normed * jnp.mean(back_n * normed, axis=1, keepdims=True))
    param_total = float(3 * NE * D * FF + D)
    local_sq = (
        jnp.sum(grad_gate * grad_gate) + jnp.sum(grad_up * grad_up) + jnp.sum(grad_down * grad_down)
    )
    count_all, gain_all, squares_all = lax.psum(
        (local_count, gain_local, local_sq), ("dp", "expert")
    )
    count = jnp.maximum(count_all, 1.0)
    gain_grad = gain_all / count
    total = squares_all / (count * count) + jnp.sum(gain_grad * gain_grad)
    factor = 1.0 / jnp.maximum(jnp.sqrt(total / param_total), 1.0)
    scale = factor / count
    grad_residual = grad_core / count
    gate_update = (grad_gate * scale).astype(jnp.bfloat16)
    up_update = (grad_up * scale).astype(jnp.bfloat16)
    down_update = (grad_down * scale).astype(jnp.bfloat16)
    return (grad_residual, gain_grad * factor, gate_update, up_update, down_update)

MESH = pl.DeviceIdType.MESH
VMEM = pl.BlockSpec(memory_space=pltpu.VMEM)
HBM = pl.BlockSpec(memory_space=pl.ANY)
NT = (((1,), (1,)), ((), ()))
F32 = dict(preferred_element_type=jnp.float32)
LOADS = 4
STEPS = 8
SLOTS = 4


def front_kernel(
    n_dp, n_expert, param_total, chunk,
    res_ref, grad_ref, routes_ref, gates_ref, valid_ref, keep_ref, gain_ref,
    wg_ref, wu_ref, wd_ref,
    core_out, gain_out, scale_out, xt_out, c_out, dgu_out, ht_out,
    gu, wd, rows, land_x, land_g, land_m, x_ref, normed, pre, back_h, hid_ref, back,
    c_ref, dgu_ref, xt_ref, ht_ref,
    land_eb, stage, land_row, msg, land_msg, land_gain, gain_part,
    w_sem, d_sem, o_sem, x_send, x_recv, x_cross, m_sem,
    eb_send, eb_recv, row_send, row_recv, g_sem,
):
    n = n_dp * n_expert
    d, e = lax.axis_index("dp"), lax.axis_index("expert")
    me = e * n_dp + d
    per_dev, width, two_hid = gu.shape
    hid = two_hid // 2
    lanes = width // 128
    n_chunks = width // chunk

    def place(row):
        return {"dp": row % n_dp, "expert": row // n_dp}

    others = [(me + k) % n for k in range(1, n)]
    barrier = pltpu.get_barrier_semaphore()
    for row in others:
        pl.semaphore_signal(barrier, inc=1, device_id=place(row), device_id_type=MESH)

    def load_gu(l, p):
        size = width // LOADS
        at = pl.ds(p * size, size)
        return (
            pltpu.make_async_copy(wg_ref.at[l, at, :], gu.at[l, at, pl.ds(0, hid)], w_sem.at[l, 0, p]),
            pltpu.make_async_copy(wu_ref.at[l, at, :], gu.at[l, at, pl.ds(hid, hid)], w_sem.at[l, 1, p]),
        )

    def load_wd(l, p):
        size = hid // LOADS
        at = pl.ds(p * size, size)
        return pltpu.make_async_copy(wd_ref.at[l, at, :], wd.at[at, :], d_sem.at[l, p])

    def start_gu(l):
        for p in range(LOADS):
            for copy in load_gu(l, p):
                copy.start()

    def wait_gu(l):
        for p in range(LOADS):
            for copy in load_gu(l, p):
                copy.wait()

    def start_wd(l):
        for p in range(LOADS):
            load_wd(l, p).start()

    def wait_wd(l):
        for p in range(LOADS):
            load_wd(l, p).wait()

    start_gu(0)
    start_wd(0)

    wide = res_ref[...].astype(jnp.float32)
    inv_rms = lax.rsqrt(jnp.mean(wide * wide, axis=1, keepdims=True) + norm_eps)
    grad = grad_ref[...].astype(jnp.float32)
    for j in range(lanes):
        at = slice(j * 128, (j + 1) * 128)
        rows[j : j + 1, :] = wide[:, at]
        rows[lanes + j : lanes + j + 1, :] = grad[:, at]
    land_x[me] = rows[:lanes].astype(jnp.bfloat16)
    land_g[me] = rows[lanes : 2 * lanes].astype(jnp.bfloat16)
    lane = lax.broadcasted_iota(jnp.int32, (1, 128), 1)
    parts = (
        routes_ref[:, 0:1].astype(jnp.float32),
        routes_ref[:, 1:2].astype(jnp.float32),
        gates_ref[:, 0:1],
        gates_ref[:, 1:2],
        (valid_ref[...] * keep_ref[...]).astype(jnp.float32),
        inv_rms,
    )
    meta = jnp.zeros((1, 128), jnp.float32)
    for at, part in enumerate(parts):
        meta = jnp.where(lane == at, part, meta)
    land_m[me] = meta

    pl.semaphore_wait(barrier, n - 1)

    def remote(src, dst, send, recv, where):
        return pltpu.make_async_remote_copy(
            src_ref=src, dst_ref=dst, send_sem=send, recv_sem=recv,
            device_id=where, device_id_type=MESH,
        )

    half = n_expert // 2
    mate = e + 1 - 2 * (e % 2)
    same = [
        ((d + k // half) % n_dp, (e + 2 * (k % half)) % n_expert) for k in range(1, n_dp * half)
    ]
    lands = (land_x, land_g)

    def direct(i, k, row):
        pd, pe = same[k]
        at = lands[i].at[row]
        return remote(at, at, x_send.at[i], x_recv.at[i, row], {"dp": pd, "expert": pe})

    def forward(i, row):
        at = lands[i].at[row]
        return remote(at, at, x_send.at[i], x_cross.at[i], {"expert": mate})

    def many(ref, count, send, recv):
        at = ref.at[pl.ds(0, count)]
        return remote(at, at, send, recv, {"expert": mate})

    def meta_copy(k):
        return remote(land_m.at[me], land_m.at[me], m_sem.at[0], m_sem.at[1], place(others[k]))

    for i in range(2):
        for k in range(len(same)):
            direct(i, k, me).start()
        forward(i, me).start()
        if i == 0:
            for k in range(n - 1):
                meta_copy(k).start()

    def relay(i, some):
        for k in some:
            pd, pe = same[k]
            row = pe * n_dp + pd
            direct(i, k, row).wait_recv()
            forward(i, row).start()

    def finish(i):
        many(lands[i], len(same) + 1, x_send.at[i], x_cross.at[i]).wait_recv()

    middle = len(same) // 2
    relay(0, range(middle))
    wait_gu(0)
    wait_wd(0)
    for l in range(1, per_dev):
        start_gu(l)
    relay(0, range(middle, len(same)))
    many(land_m, n - 1, m_sem.at[0], m_sem.at[1]).wait_recv()
    finish(0)
    relay(1, range(len(same)))

    meta_all = land_m[:, 0, :]
    inv_all = meta_all[:, 5:6]
    pitch = lanes + 1

    def spread(land):
        for r in range(n):
            rows[r * pitch : r * pitch + lanes, :] = land[r].astype(jnp.float32)

    spread(land_x)
    for j in range(lanes):
        at = slice(j * 128, (j + 1) * 128)
        part = rows[pl.ds(j, n, stride=pitch), :] * inv_all
        normed[:, at] = part
        x_ref[:, at] = (part * gain_ref[:, at]).astype(jnp.bfloat16)

    out_copies = [
        pltpu.make_async_copy(src, dst, o_sem.at[i])
        for i, (src, dst) in enumerate(
            ((c_ref, c_out), (dgu_ref, dgu_out), (ht_ref, ht_out), (xt_ref, xt_out))
        )
    ]

    for l in range(per_dev):
        if l > 0:
            wait_gu(l)
        pre[...] = jnp.dot(x_ref[...], gu[l], **F32)
        if l == 0:
            finish(1)
            spread(land_g)
            alive = meta_all[:, 4:5] > 0
            weights = []
            for k in range(per_dev):
                own = (e * per_dev + k).astype(jnp.float32)
                weights.append(
                    jnp.where(meta_all[:, 0:1] == own, meta_all[:, 2:3], 0.0)
                    + jnp.where(meta_all[:, 1:2] == own, meta_all[:, 3:4], 0.0)
                )
            for j in range(lanes):
                at = slice(j * 128, (j + 1) * 128)
                part = jnp.where(alive, rows[pl.ds(j, n, stride=pitch), :], 0.0)
                for k in range(per_dev):
                    c_ref[k, :, at] = (weights[k] * part).astype(jnp.bfloat16)
            out_copies[0].start()
        else:
            wait_wd(l)
        back_h[...] = lax.dot_general(c_ref[l], wd[...], NT, **F32)
        if l + 1 < per_dev:
            start_wd(l + 1)
        for j in range(hid // 128):
            at = slice(j * 128, (j + 1) * 128)
            up_at = slice(hid + j * 128, hid + (j + 1) * 128)
            gate_pre, up_pre, down_in = pre[:, at], pre[:, up_at], back_h[:, at]
            sigma = jax.nn.sigmoid(gate_pre)
            active = gate_pre * sigma
            hid_ref[l, :, at] = (active * up_pre).astype(jnp.bfloat16)
            dgu_ref[l, :, up_at] = (down_in * active).astype(jnp.bfloat16)
            dgu_ref[l, :, at] = (
                down_in * up_pre * sigma * (1.0 + gate_pre * (1.0 - sigma))
            ).astype(jnp.bfloat16)
    out_copies[1].start()

    mine = pl.multiple_of(e * n_dp, n_dp)

    def span(ci):
        return pl.ds(pl.multiple_of(ci * chunk, chunk), chunk)

    def eb_copy(ci, pe, slot):
        return remote(
            back.at[pl.ds(pl.multiple_of(pe * n_dp, n_dp), n_dp), span(ci)],
            land_eb.at[slot, :, span(ci)], eb_send.at[ci, pe], eb_recv.at[ci, slot], {"expert": pe},
        )

    def row_copy(ci, pd, slot):
        return remote(
            stage.at[pd, :, span(ci)], land_row.at[slot, :, span(ci)],
            row_send.at[ci, pd], row_recv.at[ci, slot], {"dp": pd},
        )

    e_peers = [(e + k) % n_expert for k in range(1, n_expert)]
    d_peers = [(d + k) % n_dp for k in range(1, n_dp)]

    def fold(ci):
        for pe in e_peers:
            eb_copy(ci, pe, pe).wait_recv()
        group = jnp.sum(land_eb[:, :, span(ci)], axis=0)
        for k in range(n_dp):
            stage[k, :, span(ci)] = group[k : k + 1]
        land_row[d, :, span(ci)] = stage[d, :, span(ci)]
        for pd in d_peers:
            row_copy(ci, pd, d).start()

    def back_step(ci, _):
        part = lax.dot_general(dgu_ref[0], gu[0, span(ci), :], NT, **F32)
        for l in range(1, per_dev):
            part += lax.dot_general(dgu_ref[l], gu[l, span(ci), :], NT, **F32)
        back[:, span(ci)] = part
        gain_part[:, span(ci)] = jnp.sum(part * normed[:, span(ci)], axis=0, keepdims=True)
        land_eb[e, :, span(ci)] = back[pl.ds(mine, n_dp), span(ci)]
        for pe in e_peers:
            eb_copy(ci, pe, e).start()

        @pl.when(ci >= 1)
        def _():
            fold(ci - 1)

        return 0

    lax.fori_loop(0, n_chunks, back_step, 0)

    piece = width // n
    for k in range(n):
        msg[k] = gain_part[:, k * piece : (k + 1) * piece]

    def msg_copy(k):
        return remote(msg.at[others[k]], land_msg.at[me], g_sem.at[0], g_sem.at[1], place(others[k]))

    def gain_copy(k):
        return remote(land_gain.at[me], land_gain.at[me], g_sem.at[2], g_sem.at[3], place(others[k]))

    for k in range(n - 1):
        msg_copy(k).start()
    land_msg[me] = msg[me]
    fold(n_chunks - 1)
    gram_x = lax.dot_general(x_ref[...], x_ref[...], NT, **F32)
    squares = jnp.zeros((1, 1), jnp.float32)
    for l in range(per_dev):
        dgu, hidden, c = dgu_ref[l], hid_ref[l], c_ref[l]
        terms = lax.dot_general(dgu, dgu, NT, **F32) * gram_x + lax.dot_general(
            hidden, hidden, NT, **F32
        ) * lax.dot_general(c, c, NT, **F32)
        squares += jnp.sum(jnp.sum(terms, axis=1, keepdims=True), axis=0, keepdims=True)
        ht_ref[l] = hidden.T
    out_copies[2].start()
    xt_ref[...] = x_ref[...].T
    out_copies[3].start()
    many(land_msg, n - 1, g_sem.at[0], g_sem.at[1]).wait_recv()
    land_gain[me, :, :piece] = jnp.sum(land_msg[...], axis=0)
    land_gain[me, :, piece:] = jnp.broadcast_to(squares, (1, 128))
    for k in range(n - 1):
        gain_copy(k).start()

    count = jnp.maximum(jnp.sum(land_m[:, :, 4:5]), 1.0)
    for i, land in enumerate(lands):
        many(land, n - 1, x_send.at[i], x_cross.at[i]).wait_send()
    many(land_m, n - 1, m_sem.at[0], m_sem.at[1]).wait_send()
    many(land_msg, n - 1, g_sem.at[0], g_sem.at[1]).wait_send()
    for ci in range(n_chunks):
        for pe in e_peers:
            eb_copy(ci, pe, e).wait_send()
        for pd in d_peers:
            row_copy(ci, pd, d).wait_send()
    for ci in range(n_chunks):
        for pd in d_peers:
            row_copy(ci, pd, pd).wait_recv()
    own_wide = res_ref[...].astype(jnp.float32)
    own_inv = lax.rsqrt(jnp.mean(own_wide * own_wide, axis=1, keepdims=True) + norm_eps)
    own_normed = own_wide * own_inv
    back_n = jnp.sum(land_row[...], axis=0) * gain_ref[...]
    core = own_inv * (back_n - own_normed * jnp.mean(back_n * own_normed, axis=1, keepdims=True))
    core_out[...] = core / count
    for copy in out_copies:
        copy.wait()

    many(land_gain, n - 1, g_sem.at[2], g_sem.at[3]).wait_recv()
    gain_grad = land_gain[:, :, :piece] / count
    squares_all = jnp.sum(land_gain[:, :, piece : piece + 1])
    whole = squares_all / (count * count) + jnp.sum(gain_grad * gain_grad)
    factor = 1.0 / jnp.maximum(jnp.sqrt(whole / param_total), 1.0)
    gain_out[...] = gain_grad * factor
    scale_out[...] = jnp.broadcast_to(factor / count, scale_out.shape)
    many(land_gain, n - 1, g_sem.at[2], g_sem.at[3]).wait_send()


def update_kernel(
    core_ref, gain_ref, scale_ref, xt_hbm, c_hbm, dgu_hbm, ht_hbm,
    resid_out, gain_out, og_ref, ou_ref, od_ref,
    xt_ref, c_ref, dgu_ref, ht_ref, buf, buf_d, in_sem, sem, sem_d,
):
    per_dev, width, hid = og_ref.shape
    slots, _, size, _ = buf.shape
    size_d = buf_d.shape[1]
    loads = [
        pltpu.make_async_copy(src, dst, in_sem.at[i])
        for i, (src, dst) in enumerate(
            ((xt_hbm, xt_ref), (dgu_hbm, dgu_ref), (ht_hbm, ht_ref), (c_hbm, c_ref))
        )
    ]
    for load in loads:
        load.start()
    resid_out[...] = core_ref[...]
    piece = gain_ref.shape[2]
    for k in range(gain_ref.shape[0]):
        gain_out[:, k * piece : (k + 1) * piece] = gain_ref[k]
    scale = scale_ref[:, 0:1]
    total = per_dev * STEPS

    def copies(t):
        l, i, s = t // STEPS, t % STEPS, t % slots
        at = pl.ds(pl.multiple_of(i * size, size), size)
        at_d = pl.ds(pl.multiple_of(i * size_d, size_d), size_d)
        return (
            pltpu.make_async_copy(buf.at[s, 0], og_ref.at[l, at, :], sem.at[s, 0]),
            pltpu.make_async_copy(buf.at[s, 1], ou_ref.at[l, at, :], sem.at[s, 1]),
            pltpu.make_async_copy(buf_d.at[s], od_ref.at[l, at_d, :], sem_d.at[s]),
        )

    def body(t, _):
        l, i, s = t // STEPS, t % STEPS, t % slots

        @pl.when(t >= slots)
        def _():
            for copy in copies(t - slots):
                copy.wait()

        at_rows = pl.ds(pl.multiple_of(i * size, size), size)
        for at in range(0, 2 * hid, 256):
            part = jnp.dot(xt_ref[at_rows, :], dgu_ref[l, :, at : at + 256], **F32) * scale
            part = part.astype(jnp.bfloat16)
            for k in range(0, 256, 128):
                col = at + k
                buf[s, col // hid, :, col % hid : col % hid + 128] = part[:, k : k + 128]
        gate_copy, up_copy, down_copy = copies(t)
        gate_copy.start()
        up_copy.start()

        at_rows = pl.ds(pl.multiple_of(i * size_d, size_d), size_d)
        for at in range(0, width, 256):
            part = jnp.dot(ht_ref[l, at_rows, :], c_ref[l, :, at : at + 256], **F32) * scale
            buf_d[s, :, at : at + 256] = part.astype(jnp.bfloat16)
        down_copy.start()
        return 0

    for load in loads:
        load.wait()
    lax.fori_loop(0, total, body, 0)
    for t in range(total - slots, total):
        for copy in copies(t):
            copy.wait()


def shards_kernel(
    n_dp,
    n_expert,
    residual,
    norm_gain,
    w_gate,
    w_up,
    w_down,
    routes,
    gate_weights,
    valid_mask,
    keep_group,
    grad_out,
):
    n = n_dp * n_expert
    per_dev, width, hid = w_gate.shape
    lanes = width // 128
    piece = width // n
    chunk = width // 4
    n_chunks = width // chunk
    param_total = float(3 * n_expert * per_dev * width * hid * n_dp + width)
    bf = lambda *shape: pltpu.VMEM(shape, jnp.bfloat16)
    vec = lambda *shape: pltpu.VMEM(shape, jnp.float32)
    dma = lambda *shape: pltpu.SemaphoreType.DMA(shape)
    shape_bf = lambda *shape: jax.ShapeDtypeStruct(shape, jnp.bfloat16)
    shape_f = lambda *shape: jax.ShapeDtypeStruct(shape, jnp.float32)
    core, gain, scale, xt, c, dgu, ht = pl.pallas_call(
        functools.partial(front_kernel, n_dp, n_expert, param_total, chunk),
        out_shape=(
            shape_f(1, width),
            shape_f(n, 1, piece),
            shape_f(1, 128),
            shape_bf(width, n),
            shape_bf(per_dev, n, width),
            shape_bf(per_dev, n, 2 * hid),
            shape_bf(per_dev, hid, n),
        ),
        in_specs=[VMEM] * 7 + [HBM] * 3,
        out_specs=[VMEM] * 3 + [HBM] * 4,
        scratch_shapes=[
            bf(per_dev, width, 2 * hid),
            bf(hid, width),
            vec(n * (lanes + 1), 128),
            bf(n, lanes, 128),
            bf(n, lanes, 128),
            vec(n, 1, 128),
            bf(n, width),
            vec(n, width),
            vec(n, 2 * hid),
            vec(n, hid),
            bf(per_dev, n, hid),
            vec(n, width),
            bf(per_dev, n, width),
            bf(per_dev, n, 2 * hid),
            bf(width, n),
            bf(per_dev, hid, n),
            vec(n_expert, n_dp, width),
            vec(n_dp, 1, width),
            vec(n_dp, 1, width),
            vec(n, 1, piece),
            vec(n, 1, piece),
            vec(n, 1, piece + 128),
            vec(1, width),
            dma(per_dev, 2, LOADS),
            dma(per_dev, LOADS),
            dma(4),
            dma(2),
            dma(2, n),
            dma(2),
            dma(2),
            dma(n_chunks, n_expert),
            dma(n_chunks, n_expert),
            dma(n_chunks, n_dp),
            dma(n_chunks, n_dp),
            dma(4),
        ],
        compiler_params=pltpu.CompilerParams(
            collective_id=0, has_side_effects=True, vmem_limit_bytes=60000 * 1024
        ),
        name="front",
    )(
        residual,
        grad_out,
        routes,
        gate_weights,
        valid_mask[None],
        keep_group[None],
        norm_gain[None],
        w_gate,
        w_up,
        w_down,
    )
    size, size_d = width // STEPS, hid // STEPS
    grad_residual, gain_update, gate_update, up_update, down_update = pl.pallas_call(
        update_kernel,
        out_shape=(
            shape_f(1, width),
            shape_f(1, width),
            jax.ShapeDtypeStruct(w_gate.shape, jnp.bfloat16),
            jax.ShapeDtypeStruct(w_up.shape, jnp.bfloat16),
            jax.ShapeDtypeStruct(w_down.shape, jnp.bfloat16),
        ),
        in_specs=[VMEM] * 3 + [HBM] * 4,
        out_specs=[VMEM] * 2 + [HBM] * 3,
        scratch_shapes=[
            bf(width, n),
            bf(per_dev, n, width),
            bf(per_dev, n, 2 * hid),
            bf(per_dev, hid, n),
            bf(SLOTS, 2, size, hid),
            bf(SLOTS, size_d, width),
            dma(4),
            dma(SLOTS, 2),
            dma(SLOTS),
        ],
        compiler_params=pltpu.CompilerParams(vmem_limit_bytes=60000 * 1024),
        name="update",
    )(core, gain, scale, xt, c, dgu, ht)
    return (grad_residual, gain_update.reshape(width), gate_update, up_update, down_update)


def shards_for(mesh):
    n_dp, n_expert = mesh.shape["dp"], mesh.shape["expert"]

    def run(*args):
        residual, w_gate = args[0], args[2]
        per_dev, width, hid = w_gate.shape
        n = n_dp * n_expert
        fits = (
            residual.shape[0] == 1
            and hid % 128 == 0
            and n <= 64
            and n_dp % 8 == 0
            and n_expert % 2 == 0
            and width % (128 * n) == 0
            and width % 1024 == 0
            and (2 * per_dev + 1) * width * hid * 2 <= 50 * 2**20
        )
        if fits:
            return shards_kernel(n_dp, n_expert, *args)
        return shards_plain(*args)

    return run


def solution(mesh):
    placed = (
        P(("dp", "expert"), None),
        P(),
        P("expert", None, "dp"),
        P("expert", None, "dp"),
        P("expert", "dp", None),
        P(("dp", "expert"), None),
        P(("dp", "expert"), None),
        P(("dp", "expert")),
        P("dp"),
        P(("dp", "expert"), None),
    )
    return jax.shard_map(
        shards_for(mesh),
        mesh=mesh,
        in_specs=placed,
        out_specs=(
            P(("dp", "expert"), None),
            P(),
            P("expert", None, "dp"),
            P("expert", None, "dp"),
            P("expert", "dp", None),
        ),
        check_vma=False,
    )
```
